16 devices in a mesh: rep: 4 (over y, z, core), dp: 4 (over x).
Axes of the slice: x: 4, y: 2, z: 1, core: 2. Of those that a mesh axis runs over, the one named last changes fastest.
The devices are a block of a 4x4x8 slice.
Arguments:
- x: bfloat16 [16, 2048, 640], P(('rep', 'dp')), parts along dimension 0
- dy: bfloat16 [16, 2048, 640], P(('rep', 'dp')), parts along dimension 0
- wq: bfloat16 [2, 640, 1536], P(None, 'dp')
- wk: bfloat16 [2, 640, 128], P(None, 'dp')
- wv: bfloat16 [2, 640, 128], P(None, 'dp')
- wo: bfloat16 [2, 1536, 640], P(None, 'dp')
- w_gate: bfloat16 [2, 640, 1536], P(None, 'dp')
- w_up: bfloat16 [2, 640, 1536], P(None, 'dp')
- w_down: bfloat16 [2, 1536, 640], P(None, 'dp')
- m_wq: float32 [2, 640, 1536], P(None, 'dp')
- m_wk: float32 [2, 640, 128], P(None, 'dp')
- m_wv: float32 [2, 640, 128], P(None, 'dp')
- m_wo: float32 [2, 1536, 640], P(None, 'dp')
- m_w_gate: float32 [2, 640, 1536], P(None, 'dp')
- m_w_up: float32 [2, 640, 1536], P(None, 'dp')
- m_w_down: float32 [2, 1536, 640], P(None, 'dp')
- v_wq: float32 [2, 640, 1536], P(None, 'dp')
- v_wk: float32 [2, 640, 128], P(None, 'dp')
- v_wv: float32 [2, 640, 128], P(None, 'dp')
- v_wo: float32 [2, 1536, 640], P(None, 'dp')
- v_w_gate: float32 [2, 640, 1536], P(None, 'dp')
- v_w_up: float32 [2, 640, 1536], P(None, 'dp')
- v_w_down: float32 [2, 1536, 640], P(None, 'dp')
Outputs:
- output 1: bfloat16 [8, 640, 1536], P('rep', 'dp'), parts along dimension 0
- output 2: bfloat16 [8, 640, 128], P('rep', 'dp'), parts along dimension 0
- output 3: bfloat16 [8, 640, 128], P('rep', 'dp'), parts along dimension 0
- output 4: bfloat16 [8, 1536, 640], P('rep', 'dp'), parts along dimension 0
- output 5: bfloat16 [8, 640, 1536], P('rep', 'dp'), parts along dimension 0
- output 6: bfloat16 [8, 640, 1536], P('rep', 'dp'), parts along dimension 0
- output 7: bfloat16 [8, 1536, 640], P('rep', 'dp'), parts along dimension 0
- output 8: float32 [8, 640, 1536], P('rep', 'dp'), parts along dimension 0
- output 9: float32 [8, 640, 128], P('rep', 'dp'), parts along dimension 0
- output 10: float32 [8, 640, 128], P('rep', 'dp'), parts along dimension 0
- output 11: float32 [8, 1536, 640], P('rep', 'dp'), parts along dimension 0
- output 12: float32 [8, 640, 1536], P('rep', 'dp'), parts along dimension 0
- output 13: float32 [8, 640, 1536], P('rep', 'dp'), parts along dimension 0
- output 14: float32 [8, 1536, 640], P('rep', 'dp'), parts along dimension 0
- output 15: float32 [8, 640, 1536], P('rep', 'dp'), parts along dimension 0
- output 16: float32 [8, 640, 128], P('rep', 'dp'), parts along dimension 0
- output 17: float32 [8, 640, 128], P('rep', 'dp'), parts along dimension 0
- output 18: float32 [8, 1536, 640], P('rep', 'dp'), parts along dimension 0
- output 19: float32 [8, 640, 1536], P('rep', 'dp'), parts along dimension 0
- output 20: float32 [8, 640, 1536], P('rep', 'dp'), parts along dimension 0
- output 21: float32 [8, 1536, 640], P('rep', 'dp'), parts along dimension 0
There are 4 independent parts. The reference program is written for one: setup_inputs(seed, part) draws one part's arguments, and reference() takes and returns one part's arrays. A program takes and returns all parts, laid end to end along the dimension named above; an argument that names none is the same for every part.
All inputs are finite; a program needn't handle non-finite values.
Results may differ from the reference program's by a relative error of at most 0.0346.
Values are sent between devices in bfloat16 or wider.
A program may use at most 768 MiB of HBM per device.

```python
import jax
import jax.numpy as jnp
from jax import lax

SEQUENCES = 4
TOKENS = 2048
D = 640
HEADS = 12
KV_HEADS = 1
HEAD = 128
FF = 1536
LAYERS = 2
THETA = 10000
NAMES = ("wq", "wk", "wv", "wo", "w_gate", "w_up", "w_down")
SHAPES = {
    "wq": (LAYERS, D, HEADS * HEAD),
    "wk": (LAYERS, D, KV_HEADS * HEAD),
    "wv": (LAYERS, D, KV_HEADS * HEAD),
    "wo": (LAYERS, HEADS * HEAD, D),
    "w_gate": (LAYERS, D, FF),
    "w_up": (LAYERS, D, FF),
    "w_down": (LAYERS, FF, D),
}


def bump(key, n, height):
    away = (jnp.arange(n, dtype=jnp.int32) - jax.random.randint(key, (), 0, n, jnp.int32)) % n
    return jnp.where(away < n // 8, height, 1.0)


def together(key, own, strength):
    shared = jax.random.normal(key, own.shape[1:], jnp.float32)
    return (own + strength * shared) * lax.rsqrt(1 + strength * strength)


def setup_inputs(seed: int = 0, part: int = 0) -> dict:
    kx, kdy, ka, kb, kz, kf, kh, kl, *keys = jax.random.split(jax.random.key(seed), 8 + 3 * len(NAMES))
    kx, kdy, ka, kb = (jax.random.fold_in(k, part) for k in (kx, kdy, ka, kb))
    kw, km, kv = (keys[i::3] for i in range(3))
    shape = (SEQUENCES, TOKENS, D)
    much_x, much_dy = jax.random.uniform(kz, (2,), jnp.float32, 0.0, 1.0)
    loud = 2.0 ** jax.random.uniform(jax.random.fold_in(kz, 1), (), jnp.float32, -1.0, 2.0)
    layers = 2.0 ** jax.random.uniform(kl, (LAYERS, 1, 1), jnp.float32, -1.0, 1.0)
    times = {"wq": 1.0, "wk": 1.0, "wv": 2.0, "wo": layers, "w_gate": 1.0, "w_up": bump(kh, FF, 4.0), "w_down": layers}
    x = together(ka, jax.random.normal(kx, shape, jnp.float32), much_x) * bump(kf, D, 4.0)
    dy = together(kb, jax.random.normal(kdy, shape, jnp.float32), much_dy)
    drawn = {"x": x.astype(jnp.bfloat16), "dy": (loud * dy * (SEQUENCES * TOKENS) ** -0.5).astype(jnp.bfloat16)}
    for key, name in zip(kw, NAMES, strict=True):
        drawn[name] = (jax.random.normal(key, SHAPES[name], jnp.float32) * SHAPES[name][1] ** -0.5 * times[name]).astype(jnp.bfloat16)
    for key, name in zip(km, NAMES, strict=True):
        drawn[f"m_{name}"] = 0.1 * jax.random.normal(key, SHAPES[name], jnp.float32)
    for key, name in zip(kv, NAMES, strict=True):
        drawn[f"v_{name}"] = loud * loud * jax.random.uniform(key, SHAPES[name], jnp.float32, 0.2, 0.6)
    return drawn


def matmul(a, w):
    return jnp.dot(a, w, preferred_element_type=jnp.float32).astype(jnp.bfloat16)


def normed(h):
    wide = h.astype(jnp.float32)
    scale = lax.rsqrt(jnp.mean(wide**2, -1, keepdims=True) + 1e-6)
    return (wide * scale).astype(jnp.bfloat16)


def turned(t, theta):
    half = t.shape[-1] // 2
    angle = jnp.arange(t.shape[0], dtype=jnp.float32)[:, None] * theta ** (-jnp.arange(half, dtype=jnp.float32) / half)
    cos, sin = jnp.cos(angle)[:, None], jnp.sin(angle)[:, None]
    a, b = t[..., :half].astype(jnp.float32), t[..., half:].astype(jnp.float32)
    return jnp.concatenate([a * cos - b * sin, b * cos + a * sin], -1).astype(jnp.bfloat16)


def seen_by(q, k, v):
    tokens, kv = q.shape[0], k.shape[1]
    q = q.reshape(tokens, kv, -1, q.shape[-1])
    scores = jnp.einsum("tgsd,ugd->gstu", q.astype(jnp.float32), k.astype(jnp.float32)) * q.shape[-1] ** -0.5
    place = jnp.arange(tokens)
    weights = jax.nn.softmax(jnp.where(place[:, None] >= place, scores, -jnp.inf), -1).astype(jnp.bfloat16)
    return jnp.einsum("gstu,ugd->tgsd", weights.astype(jnp.float32), v.astype(jnp.float32)).astype(jnp.bfloat16).reshape(tokens, -1)


def layer(h, w):
    a = normed(h)
    q, k = (turned(matmul(a, w[name]).reshape(h.shape[0], -1, HEAD), THETA) for name in ("wq", "wk"))
    h = h + matmul(seen_by(q, k, matmul(a, w["wv"]).reshape(h.shape[0], -1, HEAD)), w["wo"])
    b = normed(h)
    gate = jnp.dot(b, w["w_gate"], preferred_element_type=jnp.float32)
    up = jnp.dot(b, w["w_up"], preferred_element_type=jnp.float32)
    return h + matmul((jax.nn.silu(gate) * up).astype(jnp.bfloat16), w["w_down"])


def adamw(w, m, v, g):
    m = 0.9 * m + 0.1 * g
    v = 0.95 * v + 0.05 * g * g
    step = m * lax.rsqrt(v + 1e-8) + 0.1 * w
    return (w - 0.02 * step).astype(jnp.bfloat16), m, v


def stack(weights, h):
    return lax.scan(lambda h, w: (layer(h, w), None), h, weights)[0]


def reference(x, dy, wq, wk, wv, wo, w_gate, w_up, w_down, m_wq, m_wk, m_wv, m_wo, m_w_gate, m_w_up, m_w_down, v_wq, v_wk, v_wv, v_wo, v_w_gate, v_w_up, v_w_down):
    weights = dict(zip(NAMES, (wq, wk, wv, wo, w_gate, w_up, w_down), strict=True))

    def take(so_far, sequence):
        h, by_y = sequence
        _, back = jax.vjp(stack, weights, h)
        by_weights, by_h = back(by_y)
        return jax.tree.map(lambda total, term: total + term.astype(jnp.float32), so_far, by_weights), by_h

    none_yet = {name: jnp.zeros(w.shape, jnp.float32) for name, w in weights.items()}
    by_weights, by_x = lax.scan(take, none_yet, (x, dy))
    gradients = [by_weights[name].astype(jnp.bfloat16).astype(jnp.float32) for name in NAMES]
    first = (m_wq, m_wk, m_wv, m_wo, m_w_gate, m_w_up, m_w_down)
    second = (v_wq, v_wk, v_wv, v_wo, v_w_gate, v_w_up, v_w_down)
    new = [adamw(weights[name].astype(jnp.float32), m, v, g) for name, m, v, g in zip(NAMES, first, second, gradients, strict=True)]
    return tuple(one[which] for which in range(3) for one in new)
```

```python
import functools

import jax
import jax.numpy as jnp
from jax import lax
from jax.experimental import pallas as pl
from jax.experimental.pallas import tpu as pltpu
from jax.sharding import PartitionSpec as P

HEAD = 128
THETA = 10000
LOG2E = 1.4426950408889634
LN2 = 0.6931471805599453
SCALE = HEAD**-0.5
HIDDEN = -2e30
VMEM = 60 * 2**20
F32, BF16 = jnp.float32, jnp.bfloat16
BQ = 256
BK = 512


def _dot(a, b, ca, cb):
    return lax.dot_general(a, b, (((ca,), (cb,)), ((), ())), preferred_element_type=F32)


def _scale_of(h):
    return lax.rsqrt(jnp.mean(h * h, -1, keepdims=True) + 1e-6)


def _norm_back(h, s, d):
    return s * d - h * (s * s * s * jnp.mean(h * d, -1, keepdims=True))


def _turn(t, c, s):
    return t * c + pltpu.roll(t, HEAD // 2, 1) * s


def _turn_back(t, c, s):
    return t * c + pltpu.roll(t * s, HEAD // 2, 1)


def _rows(r, n):
    return pl.BlockSpec((r, n), lambda i: (i, 0))


def _whole(shape):
    return pl.BlockSpec(shape, lambda i: (0,) * len(shape))


def _once(shape):
    return pl.BlockSpec(shape, lambda i: (0,) * len(shape), pipeline_mode=pl.Buffered(1))


def _places():
    n = lax.axis_size("dp")
    me = lax.axis_index("dp")
    return me, lax.rem(me + 1, n), lax.rem(me + n - 1, n), lax.rem(me + 2, n)


def _send(src, dst, sems, at, to):
    return pltpu.make_async_remote_copy(src_ref=src, dst_ref=dst, send_sem=sems[0].at[at], recv_sem=sems[1].at[at], device_id={"dp": to},
                                        device_id_type=pl.DeviceIdType.MESH)


def _meet():
    _, right, left, _ = _places()
    barrier = pltpu.get_barrier_semaphore()
    for other in (right, left):
        pl.semaphore_signal(barrier, inc=1, device_id={"dp": other}, device_id_type=pl.DeviceIdType.MESH)
    pl.semaphore_wait(barrier, 2)


def _at(place, rows, first=0, some=None):
    return pl.ds(pl.multiple_of(place * rows + first, 16), rows if some is None else some)


class Fetch:
    def __init__(self, number, layer, groups, step, n):
        self.number, self.layer, self.step = number, layer, step
        self.args = [w for group in groups for w in group]
        self.parts = []
        for i, group in enumerate(groups):
            first = 0
            for w in group:
                self.parts.append((i, first, w.shape[1], w.shape[2]))
                first += w.shape[2]
        self.outs = [((n * group[0].shape[1], sum(w.shape[2] for w in group)), BF16) for group in groups]
        many = len(self.parts)
        self.scratch = [pltpu.VMEM(p[2:], BF16) for p in self.parts] + [pltpu.SemaphoreType.DMA((many, 4))] * 2 + [pltpu.SemaphoreType.DMA((many, 2))]

    def _copies(self, ins, outs, scratch):
        me, right, left, _ = _places()
        sems, local = scratch[-3:-1], scratch[-1]
        for n, (i, first, rows, columns) in enumerate(self.parts):
            src, cols = ins[n].at[self.layer], slice(first, first + columns)
            block = lambda *where: outs[i].at[_at(*where), cols]
            mine, half = block(me, rows), rows // 2
            passed, back = block(left, rows, 0, half), block(right, rows, half, half)
            yield (_send(src, mine, sems, (n, 0), right), _send(src, mine, sems, (n, 1), left), _send(passed, passed, sems, (n, 2), right),
                   _send(back, back, sems, (n, 3), left), pltpu.make_async_copy(src, scratch[n], local.at[n, 0]),
                   pltpu.make_async_copy(scratch[n], mine, local.at[n, 1]))

    def stages(self):
        return {self.step: self.forward}

    def start(self, *refs):
        _meet()
        for a, b, _, _, own, _ in self._copies(*refs):
            a.start()
            b.start()
            own.start()

    def forward(self, *refs):
        for a, b, c, d, own, out in self._copies(*refs):
            a.wait_recv()
            c.start()
            b.wait_recv()
            d.start()
            own.wait()
            out.start()

    def finish(self, *refs):
        for a, b, c, d, _, out in self._copies(*refs):
            a.wait_send()
            b.wait_send()
            c.wait()
            d.wait()
            out.wait()


class Sums:
    def __init__(self, number, arrays, step, n):
        self.number, self.step, self.args = number, step, arrays
        self.parts = [(g.shape[0] // n, g.shape[1]) for g in arrays]
        self.outs = [(p, BF16) for p in self.parts for _ in range(2)]
        many = len(self.parts)
        self.scratch = [pltpu.VMEM((r // 2, c), BF16) for r, c in self.parts for _ in range(4)]
        self.scratch += [pltpu.SemaphoreType.DMA((many, 6))] * 2 + [pltpu.SemaphoreType.DMA((many, 2))]

    def _copies(self, ins, outs, scratch):
        _, right, left, over = _places()
        sems, local = scratch[-3:-1], scratch[-1]
        for n, (rows, _) in enumerate(self.parts):
            g, (came_left, came_right), half = ins[n], outs[2 * n : 2 * n + 2], rows // 2
            in_a, in_b, a, b = scratch[4 * n : 4 * n + 4]
            part = lambda place, first: g.at[_at(place, rows, first, half), :]
            yield ((_send(part(over, 0), in_a, sems, (n, 0), right), _send(part(over, half), in_b, sems, (n, 1), left),
                    _send(part(right, half), came_left.at[pl.ds(half, half), :], sems, (n, 2), right),
                    _send(part(left, 0), came_right.at[pl.ds(0, half), :], sems, (n, 3), left),
                    _send(a, came_left.at[pl.ds(0, half), :], sems, (n, 4), right), _send(b, came_right.at[pl.ds(half, half), :], sems, (n, 5), left)),
                   (pltpu.make_async_copy(part(right, 0), a, local.at[n, 0]), pltpu.make_async_copy(part(left, half), b, local.at[n, 1])),
                   (in_a, in_b, a, b))

    def stages(self):
        return {self.step: self.add, self.step + 1: self.forward}

    def start(self, *refs):
        _meet()
        got = list(self._copies(*refs))
        for far, near, _ in got:
            far[0].start()
            far[1].start()
            near[0].start()
            near[1].start()
        for far, _, _ in got:
            far[2].start()
            far[3].start()

    def add(self, *refs):
        for far, near, (in_a, in_b, a, b) in self._copies(*refs):
            for copy, own, come, to in ((far[0], near[0], in_a, a), (far[1], near[1], in_b, b)):
                copy.wait_recv()
                own.wait()
                to[...] = (to[...].astype(F32) + come[...].astype(F32)).astype(BF16)

    def forward(self, *refs):
        for far, _, _ in self._copies(*refs):
            far[4].start()
            far[5].start()

    def finish(self, *refs):
        for far, _, _ in self._copies(*refs):
            far[0].wait_send()
            far[1].wait_send()
            for copy in far[2:]:
                copy.wait()


def _call(body, name, steps, ins, outs, scratch, args, flops, exps=0, carried=None):
    size = sum(a.size * a.dtype.itemsize for a in args) + sum(jnp.dtype(t).itemsize * functools.reduce(lambda x, y: x * y, s) for _, s, t in outs)
    args, ins, outs, scratch = list(args), list(ins), list(outs), list(scratch)
    params = dict(dimension_semantics=("arbitrary",), vmem_limit_bytes=VMEM)
    run = body
    if carried is not None:
        cuts, at = [], 0
        for many in (len(ins), len(carried.args), len(outs), len(carried.outs), len(scratch), len(carried.scratch)):
            cuts.append(slice(at, at + many))
            at += many
        args += carried.args
        ins += [pl.BlockSpec(memory_space=pl.ANY)] * len(carried.args)
        outs += [(pl.BlockSpec(memory_space=pl.ANY), *o) for o in carried.outs]
        scratch += carried.scratch
        params.update(collective_id=carried.number, has_side_effects=True)

        def run(*refs):
            own = [refs[c] for c in cuts]
            moved = own[1::2]
            i = pl.program_id(0)
            pl.when(i == 0)(lambda: carried.start(*moved))
            for at, stage in carried.stages().items():
                pl.when(i == at)(functools.partial(stage, *moved))
            body(*own[0], *own[2], *own[4])
            pl.when(i == steps - 1)(lambda: carried.finish(*moved))

    return pl.pallas_call(
        run,
        name=name,
        grid=(steps,),
        in_specs=ins,
        out_specs=[o[0] for o in outs],
        out_shape=[jax.ShapeDtypeStruct(o[1], o[2]) for o in outs],
        scratch_shapes=scratch,
        compiler_params=pltpu.CompilerParams(**params),
        cost_estimate=pl.CostEstimate(flops=flops, transcendentals=exps, bytes_accessed=size),
    )(*args)


def _qkv_kernel(h_ref, w_ref, c_ref, s_ref, q_ref, k_ref, v_ref):
    h = h_ref[...].astype(F32)
    a = (h * _scale_of(h)).astype(BF16)
    c, s = c_ref[...], s_ref[...]
    wide = q_ref.shape[1]
    y = _dot(a, w_ref[...], 1, 0)
    for at in range(0, wide, HEAD):
        t = y[:, at : at + HEAD].astype(BF16).astype(F32)
        q_ref[:, at : at + HEAD] = (_turn(t, c, s) * (SCALE * LOG2E)).astype(BF16)
    t = y[:, wide : wide + HEAD].astype(BF16).astype(F32)
    k_ref[...] = _turn(t, c, s).astype(BF16)
    v_ref[...] = y[:, wide + HEAD :].astype(BF16)


def qkv(h, w, c, s):
    t, d = h.shape
    n = w.shape[1]
    r = 512
    return _call(_qkv_kernel, "qkv", t // r, [_rows(r, d), _once((d, n)), _rows(r, HEAD), _rows(r, HEAD)],
                 [(_rows(r, n - 2 * HEAD), (t, n - 2 * HEAD), BF16), (_rows(r, HEAD), (t, HEAD), BF16), (_rows(r, HEAD), (t, HEAD), BF16)],
                 [], (h, w, c, s), 2 * t * d * n)


def _stack(to, ref, heads):
    rows = ref.shape[0]
    for n in range(heads):
        to[n * rows : (n + 1) * rows, :] = ref[:, n * HEAD : (n + 1) * HEAD]


def _attend_kernel(q_ref, k_ref, v_ref, o_ref, lse_ref, q_s, v_s, score_s, top_s, mix_s, *, heads):
    iq = pl.program_id(0)

    @pl.when(iq == 0)
    def _():
        v_s[:, :HEAD] = v_ref[...]
        v_s[:, HEAD:] = jnp.ones((v_s.shape[0], HEAD), BF16)

    _stack(q_s, q_ref, heads)
    top_s[...] = jnp.full(top_s.shape, HIDDEN, F32)
    mix_s[...] = jnp.zeros_like(mix_s)
    ok = lax.broadcasted_iota(jnp.int32, (BQ, BQ), 0) >= lax.broadcasted_iota(jnp.int32, (BQ, BQ), 1)

    def score(j, masked):
        k = k_ref[pl.ds(pl.multiple_of(j * BQ, BQ), BQ), :]
        for n in range(heads):
            rows = slice(n * BQ, (n + 1) * BQ)
            x = _dot(q_s[rows, :], k, 1, 1)
            if masked:
                x = jnp.where(ok, x, HIDDEN)
            score_s[j, rows, :] = x
            top_s[rows, :] = jnp.maximum(top_s[rows, :], jnp.maximum(x[:, :HEAD], x[:, HEAD:]))

    lax.fori_loop(0, iq, lambda j, _: score(j, False), None)
    score(iq, True)
    top_s[...] = jnp.broadcast_to(top_s[...].max(axis=1, keepdims=True), top_s.shape)

    def weigh(j, _):
        v = v_s[pl.ds(pl.multiple_of(j * BQ, BQ), BQ), :]
        for n in range(heads):
            rows = slice(n * BQ, (n + 1) * BQ)
            top = top_s[rows, :]
            p = jnp.exp2(score_s[j, rows, :] - jnp.concatenate([top, top], axis=1)).astype(BF16)
            mix_s[rows, :] += _dot(p, v, 1, 0)

    lax.fori_loop(0, iq + 1, weigh, None)
    for n in range(heads):
        rows = slice(n * BQ, (n + 1) * BQ)
        total = mix_s[rows, HEAD:]
        o_ref[:, n * HEAD : (n + 1) * HEAD] = (mix_s[rows, :HEAD] * (1 / total)).astype(BF16)
        lse_ref[n] = (top_s[rows, :] + jnp.log2(total)).T[:1, :]


def attend(q, k, v, carried):
    t, n = q.shape
    heads, steps = n // HEAD, t // BQ
    rows = heads * BQ
    return _call(functools.partial(_attend_kernel, heads=heads), "attend", steps,
                 [_rows(BQ, n), _whole((t, HEAD)), _whole((t, HEAD))],
                 [(_rows(BQ, n), (t, n), BF16), (pl.BlockSpec((heads, 1, BQ), lambda i: (0, 0, i)), (heads, 1, t), F32)],
                 [pltpu.VMEM((rows, HEAD), BF16), pltpu.VMEM((t, 2 * HEAD), BF16), pltpu.VMEM((steps, rows, BQ), F32), pltpu.VMEM((rows, HEAD), F32),
                  pltpu.VMEM((rows, 2 * HEAD), F32)],
                 (q, k, v), 2 * t * t * n, t * t * heads // 2, carried)


def _mlp_kernel(h_ref, o_ref, wo_ref, wgu_ref, wd_ref, h1_ref, h2_ref):
    h = h_ref[...].astype(F32) + _dot(o_ref[...], wo_ref[...], 1, 0).astype(BF16).astype(F32)
    h1 = h.astype(BF16)
    h1_ref[...] = h1
    h = h1.astype(F32)
    b = (h * _scale_of(h)).astype(BF16)
    ff = wd_ref.shape[0]
    gate = _dot(b, wgu_ref[:, :ff], 1, 0)
    up = _dot(b, wgu_ref[:, ff:], 1, 0)
    act = (gate * jax.nn.sigmoid(gate) * up).astype(BF16)
    h2_ref[...] = (h + _dot(act, wd_ref[...], 1, 0).astype(BF16).astype(F32)).astype(BF16)


def mlp(h, o, wo, wgu, wd, carried):
    t, d = h.shape
    n, ff = wo.shape[0], wd.shape[0]
    r = 512
    return _call(_mlp_kernel, "mlp", t // r, [_rows(r, d), _rows(r, n), _once((n, d)), _once((d, 2 * ff)), _once((ff, d))],
                 [(_rows(r, d), (t, d), BF16), (_rows(r, d), (t, d), BF16)], [], (h, o, wo, wgu, wd), 2 * t * d * (n + 3 * ff), t * ff, carried)


def _own(ref, sums):
    rows = ref.shape[0]
    ref[...] = sums[_at(lax.axis_index("dp"), rows), :]


def _mlp_back_kernel(h_ref, dy_ref, wgu_ref, wd_ref, dh_ref, dgu_ref, dd_ref, ogu_ref, od_ref, gu_s, d_s):
    i = pl.program_id(0)

    @pl.when(i == 0)
    def _():
        gu_s[...] = jnp.zeros_like(gu_s)
        d_s[...] = jnp.zeros_like(d_s)

    h = h_ref[...].astype(F32)
    s = _scale_of(h)
    b = (h * s).astype(BF16)
    dy = dy_ref[...]
    ff = wd_ref.shape[0]
    gate = _dot(b, wgu_ref[:, :ff], 1, 0)
    up = _dot(b, wgu_ref[:, ff:], 1, 0)
    sig = jax.nn.sigmoid(gate)
    silu = gate * sig
    act = (silu * up).astype(BF16)
    da = _dot(dy, wd_ref[...], 1, 1).astype(BF16).astype(F32)
    dgate = (da * up * (sig * (1 + gate * (1 - sig)))).astype(BF16)
    dup = (da * silu).astype(BF16)
    db = _dot(dgate, wgu_ref[:, :ff], 1, 1) + _dot(dup, wgu_ref[:, ff:], 1, 1)
    dh_ref[...] = (dy.astype(F32) + _norm_back(h, s, db)).astype(BF16)
    d_s[...] += _dot(act, dy, 0, 0)
    gu_s[:, :ff] += _dot(b, dgate, 0, 0)
    gu_s[:, ff:] += _dot(b, dup, 0, 0)

    @pl.when(i == pl.num_programs(0) - 1)
    def _():
        dgu_ref[...] = gu_s[...].astype(BF16)
        dd_ref[...] = d_s[...].astype(BF16)
        _own(ogu_ref, gu_s)
        _own(od_ref, d_s)


def mlp_back(h, dy, wgu, wd, n, carried):
    t, d = h.shape
    ff = wd.shape[0]
    r = 256
    return _call(_mlp_back_kernel, "mlp_back", t // r, [_rows(r, d), _rows(r, d), _once((d, 2 * ff)), _once((ff, d))],
                 [(_rows(r, d), (t, d), BF16), (_once((d, 2 * ff)), (d, 2 * ff), BF16), (_once((ff, d)), (ff, d), BF16),
                  (_once((d // n, 2 * ff)), (d // n, 2 * ff), F32), (_once((ff // n, d)), (ff // n, d), F32)],
                 [pltpu.VMEM((d, 2 * ff), F32), pltpu.VMEM((ff, d), F32)], (h, dy, wgu, wd), 16 * t * d * ff, t * ff, carried)


def _out_back_kernel(dh_ref, o_ref, wo_ref, do_ref, dw_ref, ow_ref, w_s):
    i = pl.program_id(0)

    @pl.when(i == 0)
    def _():
        w_s[...] = jnp.zeros_like(w_s)

    dh = dh_ref[...]
    do_ref[...] = _dot(dh, wo_ref[...], 1, 1).astype(BF16)
    w_s[...] += _dot(o_ref[...], dh, 0, 0)

    @pl.when(i == pl.num_programs(0) - 1)
    def _():
        dw_ref[...] = w_s[...].astype(BF16)
        _own(ow_ref, w_s)


def out_back(dh, o, wo, group):
    t, d = dh.shape
    n = o.shape[1]
    r = 512
    return _call(_out_back_kernel, "out_back", t // r, [_rows(r, d), _rows(r, n), _once((n, d))],
                 [(_rows(r, n), (t, n), BF16), (_once((n, d)), (n, d), BF16), (_once((n // group, d)), (n // group, d), F32)], [pltpu.VMEM((n, d), F32)], (dh, o, wo), 4 * t * d * n)


def _attend_back_kernel(q_ref, k_ref, v_ref, o_ref, do_ref, lse_ref, dq_ref, dk_ref, dv_ref, kt_s, q_s, do_s, delta_s, dqt_s, dk_s, dv_s, *, heads):
    iq = pl.program_id(0)

    @pl.when(iq == 0)
    def _():
        kt_s[...] = k_ref[...].astype(F32).T.astype(BF16)
        dk_s[...] = jnp.zeros_like(dk_s)
        dv_s[...] = jnp.zeros_like(dv_s)

    dqt_s[...] = jnp.zeros_like(dqt_s)
    _stack(q_s, q_ref, heads)
    _stack(do_s, do_ref, heads)
    for n in range(heads):
        head = slice(n * HEAD, (n + 1) * HEAD)
        delta_s[:, n * BQ : (n + 1) * BQ] = (do_ref[:, head].astype(F32) * o_ref[:, head].astype(F32)).T.sum(axis=0, keepdims=True)
    gap = lax.rem(lax.broadcasted_iota(jnp.int32, (BK, 2 * BQ), 1), BQ) - lax.broadcasted_iota(jnp.int32, (BK, 2 * BQ), 0)

    def block(j, masked):
        here = pl.ds(pl.multiple_of(j * BK, BK), BK)
        k, v, kt = k_ref[here, :], v_ref[here, :], kt_s[:, here]
        pairs = range(0, heads, 2)
        cols = [slice(n * BQ, (n + 2) * BQ) for n in pairs]
        scores = [_dot(k, q_s[c, :], 1, 1) for c in cols]
        dps = [_dot(v, do_s[c, :], 1, 1) for c in cols]
        ok = gap >= j * BK - iq * BQ if masked else None
        for n, c, x, dp in zip(pairs, cols, scores, dps):
            p = jnp.exp2(x - jnp.concatenate([lse_ref[n], lse_ref[n + 1]], axis=1))
            if masked:
                p = jnp.where(ok, p, 0.0)
            ds = (p * (dp - delta_s[:, c])).astype(BF16)
            dv_s[here, :] += _dot(p.astype(BF16), do_s[c, :], 1, 0)
            dk_s[here, :] += _dot(ds, q_s[c, :], 1, 0)
            dqt_s[:, c] += _dot(kt, ds, 1, 0)

    last = lax.div(iq * BQ, BK)
    lax.fori_loop(0, last, lambda j, _: block(j, False), None)
    block(last, True)
    for n in range(heads):
        dq_ref[:, n * HEAD : (n + 1) * HEAD] = (dqt_s[:, n * BQ : (n + 1) * BQ] * SCALE).T.astype(BF16)

    @pl.when(iq == pl.num_programs(0) - 1)
    def _():
        dk_ref[...] = (dk_s[...] * LN2).astype(BF16)
        dv_ref[...] = dv_s[...].astype(BF16)


def attend_back(q, k, v, o, do, lse, carried):
    t, n = q.shape
    heads, steps = n // HEAD, t // BQ
    whole = _whole((t, HEAD))
    cols = heads * BQ
    return _call(functools.partial(_attend_back_kernel, heads=heads), "attend_back", steps,
                 [_rows(BQ, n), whole, whole, _rows(BQ, n), _rows(BQ, n), pl.BlockSpec((heads, 1, BQ), lambda i: (0, 0, i))],
                 [(_rows(BQ, n), (t, n), BF16), (whole, (t, HEAD), BF16), (whole, (t, HEAD), BF16)],
                 [pltpu.VMEM((HEAD, t), BF16), pltpu.VMEM((cols, HEAD), BF16), pltpu.VMEM((cols, HEAD), BF16), pltpu.VMEM((1, cols), F32),
                  pltpu.VMEM((HEAD, cols), F32), pltpu.VMEM((t, HEAD), F32), pltpu.VMEM((t, HEAD), F32)],
                 (q, k, v, o, do, lse), 5 * t * t * n, t * t * heads // 2, carried)


def _qkv_back_kernel(h_ref, dq_ref, dk_ref, dv_ref, c_ref, s_ref, *rest, states):
    if states:
        dh_ref, w_ref, dx_ref, dw_ref, ow_ref, w_s = rest
    else:
        dw_ref, ow_ref, w_s = rest
    i = pl.program_id(0)

    @pl.when(i == 0)
    def _():
        w_s[...] = jnp.zeros_like(w_s)

    h = h_ref[...].astype(F32)
    scale = _scale_of(h)
    a = (h * scale).astype(BF16)
    c, s = c_ref[...], s_ref[...]
    parts = [_turn_back(dq_ref[:, at : at + HEAD].astype(F32), c, s).astype(BF16) for at in range(0, dq_ref.shape[1], HEAD)]
    parts += [_turn_back(dk_ref[...].astype(F32), c, s).astype(BF16), dv_ref[...]]
    d = jnp.concatenate(parts, axis=1)
    w_s[...] += _dot(a, d, 0, 0)
    if states:
        dx_ref[...] = (dh_ref[...].astype(F32) + _norm_back(h, scale, _dot(d, w_ref[...], 1, 1))).astype(BF16)

    @pl.when(i == pl.num_programs(0) - 1)
    def _():
        dw_ref[...] = w_s[...].astype(BF16)
        _own(ow_ref, w_s)


def qkv_back(h, dq, dk, dv, c, s, group, dh=None, w=None):
    t, d = h.shape
    n = dq.shape[1] + 2 * HEAD
    r = 512
    states = dh is not None
    ins = [_rows(r, d), _rows(r, n - 2 * HEAD)] + [_rows(r, HEAD)] * 4 + ([_rows(r, d), _once((d, n))] if states else [])
    outs = ([(_rows(r, d), (t, d), BF16)] if states else []) + [(_once((d, n)), (d, n), BF16), (_once((d // group, n)), (d // group, n), F32)]
    got = _call(functools.partial(_qkv_back_kernel, states=states), "qkv_back", t // r, ins, outs, [pltpu.VMEM((d, n), F32)],
                (h, dq, dk, dv, c, s) + ((dh, w) if states else ()), (4 if states else 2) * t * d * n)
    return got if states else (None, *got)


def _first_kernel(f_ref, c_ref, s_ref, *, rows):
    place = (lax.broadcasted_iota(jnp.int32, c_ref.shape, 0) + pl.program_id(0) * rows).astype(F32)
    angle = place * f_ref[...]
    c_ref[...] = jnp.cos(angle)
    s_ref[...] = jnp.sin(angle) * jnp.where(lax.broadcasted_iota(jnp.int32, s_ref.shape, 1) < HEAD // 2, -1.0, 1.0)


def first(tokens, carried):
    half = HEAD // 2
    f = THETA ** (-jnp.arange(half, dtype=F32) / half)
    r = tokens // 2
    return _call(functools.partial(_first_kernel, rows=r), "first", 2, [_whole((1, HEAD))], [(_rows(r, HEAD), (tokens, HEAD), F32)] * 2, [],
                 (jnp.concatenate([f, f])[None],), tokens * HEAD, tokens * HEAD, carried)


def last_sums(g, n):
    rows = g.shape[0] // n
    half = rows // 2
    _, right, left, over = _places()
    part = lambda place, first: lax.dynamic_slice_in_dim(g, place * rows + first, half, 0)
    up, down = [(i, (i + 1) % n) for i in range(n)], [(i, (i - 1) % n) for i in range(n)]
    in_a, in_b = lax.ppermute(part(over, 0), "dp", up), lax.ppermute(part(over, half), "dp", down)
    b_left, a_right = lax.ppermute(part(right, half), "dp", up), lax.ppermute(part(left, 0), "dp", down)
    both = lambda x, y: (x.astype(F32) + y.astype(F32)).astype(BF16)
    a_left = lax.ppermute(both(part(right, 0), in_a), "dp", up)
    b_right = lax.ppermute(both(part(left, half), in_b), "dp", down)
    return jnp.concatenate([a_left, b_left], 0), jnp.concatenate([a_right, b_right], 0)


def adamw(w, m, v, g):
    m = 0.9 * m + 0.1 * g
    v = 0.95 * v + 0.05 * g * g
    step = m * lax.rsqrt(v + 1e-8) + 0.1 * w
    return (w - 0.02 * step).astype(BF16), m, v


def solution(mesh):
    group = mesh.shape["dp"]

    def step(x, dy, *arrays):
        weights, m, v = (arrays[i : i + 7] for i in (0, 7, 14))
        wq, wk, wv, wo, wg, wu, wd = weights
        layers = wq.shape[0]
        heads = lambda n, at: Fetch(4 * n, n, [[wq, wk, wv]], at, group)
        c, s, wa = first(x.shape[1], heads(0, 1))
        h, kept = x[0], []
        for n in range(layers):
            q, k, vv = qkv(h, wa, c, s)
            o, lse, wb, wc, we = attend(q, k, vv, Fetch(4 * n + 1, n, [[wo], [wg, wu], [wd]], 6, group))
            h1, h2, *then = mlp(h, o, wb, wc, we, heads(n + 1, 2) if n + 1 < layers else None)
            kept.append((h, q, k, vv, o, lse, h1, wa, wb, wc, we))
            h, wa = h2, then[0] if then else None
        by_h, own, came, waiting = dy[0], [None] * layers, [None] * layers, None
        for n in reversed(range(layers)):
            h, q, k, vv, o, lse, h1, wa, wb, wc, we = kept[n]
            dh1, dgu, dd, ogu, od, *got = mlp_back(h1, by_h, wc, we, group, Sums(4 * n + 2, [waiting], 2, group) if n + 1 < layers else None)
            if got:
                came[n + 1] += got
            do, dwo, owo = out_back(dh1, o, wb, group)
            dq, dk, dv, *got = attend_back(q, k, vv, o, do, lse, Sums(4 * n + 3, [dwo, dgu, dd], 4, group))
            by_h, waiting, oqkv = qkv_back(h, dq, dk, dv, c, s, group, *((dh1, wa) if n else ()))
            own[n], came[n] = [owo, ogu, od, oqkv], got
        came[0] += last_sums(waiting, group)

        def sums(n):
            o, gu, d, qkv = (one + came[n][2 * i].astype(F32) + came[n][2 * i + 1].astype(F32) for i, one in enumerate(own[n]))
            a, b, ff = wq.shape[2], wk.shape[2], wg.shape[2]
            return qkv[:, :a], qkv[:, a : a + b], qkv[:, a + b :], o, gu[:, :ff], gu[:, ff:], d

        gradients = [jnp.stack(g).astype(BF16).astype(F32) for g in zip(*(sums(n) for n in range(layers)))]
        new = [adamw(w.astype(F32), m, v, g) for w, m, v, g in zip(weights, m, v, gradients, strict=True)]
        return tuple(one[which] for which in range(3) for one in new)

    states, cut = P(("rep", "dp"), None, None), P(None, "dp", None)
    return jax.shard_map(
        step,
        mesh=mesh,
        in_specs=(states, states) + (cut,) * 21,
        out_specs=(P("rep", "dp", None),) * 21,
        check_vma=False,
    )
```

```python
import functools

import jax
import jax.numpy as jnp
from jax import lax
from jax.experimental import pallas as pl
from jax.experimental.pallas import tpu as pltpu
from jax.sharding import PartitionSpec as P

HEAD = 128
THETA = 10000
LOG2E = 1.4426950408889634
LN2 = 0.6931471805599453
SCALE = HEAD**-0.5
HIDDEN = -2e30
VMEM = 60 * 2**20
F32, BF16 = jnp.float32, jnp.bfloat16
BQ = 256
BK = 256


def _dot(a, b, ca, cb):
    return lax.dot_general(a, b, (((ca,), (cb,)), ((), ())), preferred_element_type=F32)


def _scale_of(h):
    return lax.rsqrt(jnp.mean(h * h, -1, keepdims=True) + 1e-6)


def _norm_back(h, s, d):
    return s * d - h * (s * s * s * jnp.mean(h * d, -1, keepdims=True))


def _turn(t, c, s):
    return t * c + pltpu.roll(t, HEAD // 2, 1) * s


def _turn_back(t, c, s):
    return t * c + pltpu.roll(t * s, HEAD // 2, 1)


def _rows(r, n):
    return pl.BlockSpec((r, n), lambda i: (i, 0))


def _whole(shape):
    return pl.BlockSpec(shape, lambda i: (0,) * len(shape))


def _once(shape):
    return pl.BlockSpec(shape, lambda i: (0,) * len(shape), pipeline_mode=pl.Buffered(1))


def _places():
    n = lax.axis_size("dp")
    me = lax.axis_index("dp")
    return me, lax.rem(me + 1, n), lax.rem(me + n - 1, n), lax.rem(me + 2, n)


def _send(src, dst, sems, at, to):
    return pltpu.make_async_remote_copy(src_ref=src, dst_ref=dst, send_sem=sems[0].at[at], recv_sem=sems[1].at[at], device_id=to,
                                        device_id_type=pl.DeviceIdType.MESH)


def _twin():
    place = lax.axis_index("rep")
    core = lax.rem(place, 2)
    return core, place + 1 - 2 * core


def _meet(twin):
    _, right, left, _ = _places()
    barrier = pltpu.get_barrier_semaphore()
    others = [{"dp": right}, {"dp": left}] + ([{"rep": _twin()[1]}] if twin else [])
    for other in others:
        pl.semaphore_signal(barrier, inc=1, device_id=other, device_id_type=pl.DeviceIdType.MESH)
    pl.semaphore_wait(barrier, len(others))


def _at(place, rows, first=0, some=None):
    return pl.ds(pl.multiple_of(place * rows + first, 16), rows if some is None else some)


class Fetch:
    def __init__(self, number, layer, groups, steps, n):
        self.number, self.layer, self.steps = number, layer, steps
        self.args = [w for group in groups for w in group]
        self.parts = []
        for i, group in enumerate(groups):
            first = 0
            for w in group:
                self.parts.append((i, first, w.shape[1], w.shape[2]))
                first += w.shape[2]
        self.outs = [((n * group[0].shape[1], sum(w.shape[2] for w in group)), BF16) for group in groups]
        many = len(self.parts)
        self.scratch = [pltpu.VMEM(p[2:], BF16) for p in self.parts] + [pltpu.SemaphoreType.DMA((many, 7))] * 2 + [pltpu.SemaphoreType.DMA((many, 2))]

    def _copies(self, ins, outs, scratch):
        me, right, left, over = _places()
        core, other = _twin()
        right_id, left_id, twin_id = {"dp": right}, {"dp": left}, {"rep": other}
        sems, local = scratch[-3:-1], scratch[-1]
        for n, (i, first, rows, columns) in enumerate(self.parts):
            cols, half, quarter = slice(first, first + columns), rows // 2, rows // 4
            at = core * half

            def block(place, first, some):
                return outs[i].at[pl.ds(pl.multiple_of(place * rows + first, 8), some), cols]

            src = ins[n].at[self.layer]
            mine = ins[n].at[self.layer, pl.ds(pl.multiple_of(at, 8), half), :]
            to, passed, back = block(me, at, half), block(left, at, quarter), block(right, at + quarter, quarter)
            from_left, from_right, from_over = block(left, at, half), block(right, at, half), block(over, at, half)
            yield ((_send(mine, to, sems, (n, 0), right_id), _send(mine, to, sems, (n, 1), left_id), _send(passed, passed, sems, (n, 2), right_id),
                    _send(back, back, sems, (n, 3), left_id), _send(from_left, from_left, sems, (n, 4), twin_id),
                    _send(from_right, from_right, sems, (n, 5), twin_id), _send(from_over, from_over, sems, (n, 6), twin_id)),
                   (pltpu.make_async_copy(src, scratch[n], local.at[n, 0]), pltpu.make_async_copy(scratch[n], block(me, 0, rows), local.at[n, 1])))

    def stages(self):
        return {self.steps[0]: self.forward, self.steps[1]: self.share}

    def start(self, *refs):
        _meet(True)
        for far, near in self._copies(*refs):
            far[0].start()
            far[1].start()
            near[0].start()

    def forward(self, *refs):
        for far, near in self._copies(*refs):
            far[0].wait_recv()
            far[2].start()
            far[4].start()
            far[1].wait_recv()
            far[3].start()
            far[5].start()
            near[0].wait()
            near[1].start()

    def share(self, *refs):
        for far, _ in self._copies(*refs):
            far[2].wait_recv()
            far[3].wait_recv()
            far[6].start()

    def finish(self, *refs):
        for far, near in self._copies(*refs):
            for copy in far[:4]:
                copy.wait_send()
            for copy in far[4:]:
                copy.wait()
            near[1].wait()


class Sums:
    def __init__(self, number, arrays, step, n):
        self.number, self.step, self.args = number, step, arrays
        self.parts = [(g.shape[0] // n, g.shape[1]) for g in arrays]
        self.outs = [(p, BF16) for p in self.parts for _ in range(2)]
        many = len(self.parts)
        self.scratch = [pltpu.VMEM((r // 2, c), BF16) for r, c in self.parts for _ in range(4)]
        self.scratch += [pltpu.SemaphoreType.DMA((many, 6))] * 2 + [pltpu.SemaphoreType.DMA((many, 2))]

    def _copies(self, ins, outs, scratch):
        _, right, left, over = _places()
        right_id, left_id = {"dp": right}, {"dp": left}
        sems, local = scratch[-3:-1], scratch[-1]
        for n, (rows, _) in enumerate(self.parts):
            g, (came_left, came_right), half = ins[n], outs[2 * n : 2 * n + 2], rows // 2
            in_a, in_b, a, b = scratch[4 * n : 4 * n + 4]
            part = lambda place, first: g.at[_at(place, rows, first, half), :]
            yield ((_send(part(over, 0), in_a, sems, (n, 0), right_id), _send(part(over, half), in_b, sems, (n, 1), left_id),
                    _send(part(right, half), came_left.at[pl.ds(half, half), :], sems, (n, 2), right_id),
                    _send(part(left, 0), came_right.at[pl.ds(0, half), :], sems, (n, 3), left_id),
                    _send(a, came_left.at[pl.ds(0, half), :], sems, (n, 4), right_id), _send(b, came_right.at[pl.ds(half, half), :], sems, (n, 5), left_id)),
                   (pltpu.make_async_copy(part(right, 0), a, local.at[n, 0]), pltpu.make_async_copy(part(left, half), b, local.at[n, 1])),
                   (in_a, in_b, a, b))

    def stages(self):
        return {self.step: self.add, self.step + 1: self.forward}

    def start(self, *refs):
        _meet(False)
        got = list(self._copies(*refs))
        for far, near, _ in got:
            far[0].start()
            far[1].start()
            near[0].start()
            near[1].start()
        for far, _, _ in got:
            far[2].start()
            far[3].start()

    def add(self, *refs):
        for far, near, (in_a, in_b, a, b) in self._copies(*refs):
            for copy, own, come, to in ((far[0], near[0], in_a, a), (far[1], near[1], in_b, b)):
                copy.wait_recv()
                own.wait()
                to[...] = (to[...].astype(F32) + come[...].astype(F32)).astype(BF16)

    def forward(self, *refs):
        for far, _, _ in self._copies(*refs):
            far[4].start()
            far[5].start()

    def finish(self, *refs):
        for far, _, _ in self._copies(*refs):
            far[0].wait_send()
            far[1].wait_send()
            for copy in far[2:]:
                copy.wait()


def _call(body, name, steps, ins, outs, scratch, args, flops, exps=0, carried=None):
    size = sum(a.size * a.dtype.itemsize for a in args) + sum(jnp.dtype(t).itemsize * functools.reduce(lambda x, y: x * y, s) for _, s, t in outs)
    args, ins, outs, scratch = list(args), list(ins), list(outs), list(scratch)
    params = dict(dimension_semantics=("arbitrary",), vmem_limit_bytes=VMEM)
    run = body
    if carried is not None:
        cuts, at = [], 0
        for many in (len(ins), len(carried.args), len(outs), len(carried.outs), len(scratch), len(carried.scratch)):
            cuts.append(slice(at, at + many))
            at += many
        args += carried.args
        ins += [pl.BlockSpec(memory_space=pl.ANY)] * len(carried.args)
        outs += [(pl.BlockSpec(memory_space=pl.ANY), *o) for o in carried.outs]
        scratch += carried.scratch
        params.update(collective_id=carried.number, has_side_effects=True)

        def run(*refs):
            own = [refs[c] for c in cuts]
            moved = own[1::2]
            i = pl.program_id(0)
            pl.when(i == 0)(lambda: carried.start(*moved))
            for at, stage in carried.stages().items():
                pl.when(i == at)(functools.partial(stage, *moved))
            body(*own[0], *own[2], *own[4])
            pl.when(i == steps - 1)(lambda: carried.finish(*moved))

    return pl.pallas_call(
        run,
        name=name,
        grid=(steps,),
        in_specs=ins,
        out_specs=[o[0] for o in outs],
        out_shape=[jax.ShapeDtypeStruct(o[1], o[2]) for o in outs],
        scratch_shapes=scratch,
        compiler_params=pltpu.CompilerParams(**params),
        cost_estimate=pl.CostEstimate(flops=flops, transcendentals=exps, bytes_accessed=size),
    )(*args)


def _qkv_kernel(h_ref, w_ref, c_ref, s_ref, q_ref, k_ref, v_ref):
    h = h_ref[...].astype(F32)
    a = (h * _scale_of(h)).astype(BF16)
    c, s = c_ref[...], s_ref[...]
    wide = q_ref.shape[1]
    y = _dot(a, w_ref[...], 1, 0)
    for at in range(0, wide, HEAD):
        t = y[:, at : at + HEAD].astype(BF16).astype(F32)
        q_ref[:, at : at + HEAD] = (_turn(t, c, s) * (SCALE * LOG2E)).astype(BF16)
    t = y[:, wide : wide + HEAD].astype(BF16).astype(F32)
    k_ref[...] = _turn(t, c, s).astype(BF16)
    v_ref[...] = y[:, wide + HEAD :].astype(BF16)


def qkv(h, w, c, s):
    t, d = h.shape
    n = w.shape[1]
    r = 512
    return _call(_qkv_kernel, "qkv", t // r, [_rows(r, d), _once((d, n)), _rows(r, HEAD), _rows(r, HEAD)],
                 [(_rows(r, n - 2 * HEAD), (t, n - 2 * HEAD), BF16), (_rows(r, HEAD), (t, HEAD), BF16), (_rows(r, HEAD), (t, HEAD), BF16)],
                 [], (h, w, c, s), 2 * t * d * n)


def _stack(to, ref, heads):
    rows = ref.shape[0]
    for n in range(heads):
        to[n * rows : (n + 1) * rows, :] = ref[:, n * HEAD : (n + 1) * HEAD]


def _attend_kernel(q_ref, k_ref, v_ref, o_ref, lse_ref, q_s, v_s, score_s, top_s, mix_s, *, heads):
    iq = pl.program_id(0)

    @pl.when(iq == 0)
    def _():
        v_s[:, :HEAD] = v_ref[...]
        v_s[:, HEAD:] = jnp.ones((v_s.shape[0], HEAD), BF16)

    _stack(q_s, q_ref, heads)
    top_s[...] = jnp.full(top_s.shape, HIDDEN, F32)
    mix_s[...] = jnp.zeros_like(mix_s)
    ok = lax.broadcasted_iota(jnp.int32, (BQ, BQ), 0) >= lax.broadcasted_iota(jnp.int32, (BQ, BQ), 1)

    def score(j, masked):
        k = k_ref[pl.ds(pl.multiple_of(j * BQ, BQ), BQ), :]
        for n in range(heads):
            rows = slice(n * BQ, (n + 1) * BQ)
            x = _dot(q_s[rows, :], k, 1, 1)
            if masked:
                x = jnp.where(ok, x, HIDDEN)
            score_s[j, rows, :] = x
            top_s[rows, :] = jnp.maximum(top_s[rows, :], jnp.maximum(x[:, :HEAD], x[:, HEAD:]))

    lax.fori_loop(0, iq, lambda j, _: score(j, False), None)
    score(iq, True)
    top_s[...] = jnp.broadcast_to(top_s[...].max(axis=1, keepdims=True), top_s.shape)

    def weigh(j, _):
        v = v_s[pl.ds(pl.multiple_of(j * BQ, BQ), BQ), :]
        for n in range(heads):
            rows = slice(n * BQ, (n + 1) * BQ)
            top = top_s[rows, :]
            p = jnp.exp2(score_s[j, rows, :] - jnp.concatenate([top, top], axis=1)).astype(BF16)
            mix_s[rows, :] += _dot(p, v, 1, 0)

    lax.fori_loop(0, iq + 1, weigh, None)
    for n in range(heads):
        rows = slice(n * BQ, (n + 1) * BQ)
        total = mix_s[rows, HEAD:]
        o_ref[:, n * HEAD : (n + 1) * HEAD] = (mix_s[rows, :HEAD] * (1 / total)).astype(BF16)
        lse_ref[n] = (top_s[rows, :] + jnp.log2(total)).T[:1, :]


def attend(q, k, v, carried):
    t, n = q.shape
    heads, steps = n // HEAD, t // BQ
    rows = heads * BQ
    return _call(functools.partial(_attend_kernel, heads=heads), "attend", steps,
                 [_rows(BQ, n), _whole((t, HEAD)), _whole((t, HEAD))],
                 [(_rows(BQ, n), (t, n), BF16), (pl.BlockSpec((heads, 1, BQ), lambda i: (0, 0, i)), (heads, 1, t), F32)],
                 [pltpu.VMEM((rows, HEAD), BF16), pltpu.VMEM((t, 2 * HEAD), BF16), pltpu.VMEM((steps, rows, BQ), F32), pltpu.VMEM((rows, HEAD), F32),
                  pltpu.VMEM((rows, 2 * HEAD), F32)],
                 (q, k, v), 2 * t * t * n, t * t * heads // 2, carried)


def _mlp_kernel(h_ref, o_ref, wo_ref, wgu_ref, wd_ref, h1_ref, h2_ref):
    h = h_ref[...].astype(F32) + _dot(o_ref[...], wo_ref[...], 1, 0).astype(BF16).astype(F32)
    h1 = h.astype(BF16)
    h1_ref[...] = h1
    h = h1.astype(F32)
    b = (h * _scale_of(h)).astype(BF16)
    ff = wd_ref.shape[0]
    gate = _dot(b, wgu_ref[:, :ff], 1, 0)
    up = _dot(b, wgu_ref[:, ff:], 1, 0)
    act = (gate * jax.nn.sigmoid(gate) * up).astype(BF16)
    h2_ref[...] = (h + _dot(act, wd_ref[...], 1, 0).astype(BF16).astype(F32)).astype(BF16)


def mlp(h, o, wo, wgu, wd, carried):
    t, d = h.shape
    n, ff = wo.shape[0], wd.shape[0]
    r = 512
    return _call(_mlp_kernel, "mlp", t // r, [_rows(r, d), _rows(r, n), _once((n, d)), _once((d, 2 * ff)), _once((ff, d))],
                 [(_rows(r, d), (t, d), BF16), (_rows(r, d), (t, d), BF16)], [], (h, o, wo, wgu, wd), 2 * t * d * (n + 3 * ff), t * ff, carried)


def _own(ref, sums):
    rows = ref.shape[0]
    ref[...] = sums[_at(lax.axis_index("dp"), rows), :]


def _mlp_back_kernel(h_ref, dy_ref, wgu_ref, wd_ref, dh_ref, dgu_ref, dd_ref, ogu_ref, od_ref, gu_s, d_s):
    i = pl.program_id(0)

    @pl.when(i == 0)
    def _():
        gu_s[...] = jnp.zeros_like(gu_s)
        d_s[...] = jnp.zeros_like(d_s)

    h = h_ref[...].astype(F32)
    s = _scale_of(h)
    b = (h * s).astype(BF16)
    dy = dy_ref[...]
    ff = wd_ref.shape[0]
    gate = _dot(b, wgu_ref[:, :ff], 1, 0)
    up = _dot(b, wgu_ref[:, ff:], 1, 0)
    sig = jax.nn.sigmoid(gate)
    silu = gate * sig
    act = (silu * up).astype(BF16)
    da = _dot(dy, wd_ref[...], 1, 1).astype(BF16).astype(F32)
    dgate = (da * up * (sig * (1 + gate * (1 - sig)))).astype(BF16)
    dup = (da * silu).astype(BF16)
    db = _dot(dgate, wgu_ref[:, :ff], 1, 1) + _dot(dup, wgu_ref[:, ff:], 1, 1)
    dh_ref[...] = (dy.astype(F32) + _norm_back(h, s, db)).astype(BF16)
    d_s[...] += _dot(act, dy, 0, 0)
    gu_s[:, :ff] += _dot(b, dgate, 0, 0)
    gu_s[:, ff:] += _dot(b, dup, 0, 0)

    @pl.when(i == pl.num_programs(0) - 1)
    def _():
        dgu_ref[...] = gu_s[...].astype(BF16)
        dd_ref[...] = d_s[...].astype(BF16)
        _own(ogu_ref, gu_s)
        _own(od_ref, d_s)


def mlp_back(h, dy, wgu, wd, n, carried):
    t, d = h.shape
    ff = wd.shape[0]
    r = 256
    return _call(_mlp_back_kernel, "mlp_back", t // r, [_rows(r, d), _rows(r, d), _once((d, 2 * ff)), _once((ff, d))],
                 [(_rows(r, d), (t, d), BF16), (_once((d, 2 * ff)), (d, 2 * ff), BF16), (_once((ff, d)), (ff, d), BF16),
                  (_once((d // n, 2 * ff)), (d // n, 2 * ff), F32), (_once((ff // n, d)), (ff // n, d), F32)],
                 [pltpu.VMEM((d, 2 * ff), F32), pltpu.VMEM((ff, d), F32)], (h, dy, wgu, wd), 16 * t * d * ff, t * ff, carried)


def _out_back_kernel(dh_ref, o_ref, wo_ref, do_ref, dw_ref, ow_ref, w_s):
    i = pl.program_id(0)

    @pl.when(i == 0)
    def _():
        w_s[...] = jnp.zeros_like(w_s)

    dh = dh_ref[...]
    do_ref[...] = _dot(dh, wo_ref[...], 1, 1).astype(BF16)
    w_s[...] += _dot(o_ref[...], dh, 0, 0)

    @pl.when(i == pl.num_programs(0) - 1)
    def _():
        dw_ref[...] = w_s[...].astype(BF16)
        _own(ow_ref, w_s)


def out_back(dh, o, wo, group):
    t, d = dh.shape
    n = o.shape[1]
    r = 512
    return _call(_out_back_kernel, "out_back", t // r, [_rows(r, d), _rows(r, n), _once((n, d))],
                 [(_rows(r, n), (t, n), BF16), (_once((n, d)), (n, d), BF16), (_once((n // group, d)), (n // group, d), F32)], [pltpu.VMEM((n, d), F32)], (dh, o, wo), 4 * t * d * n)


def _attend_back_kernel(q_ref, k_ref, v_ref, o_ref, do_ref, lse_ref, dq_ref, dk_ref, dv_ref, kt_s, q_s, do_s, delta_s, dqt_s, dk_s, dv_s, *, heads):
    iq = pl.program_id(0)

    @pl.when(iq == 0)
    def _():
        kt_s[...] = k_ref[...].astype(F32).T.astype(BF16)
        dk_s[...] = jnp.zeros_like(dk_s)
        dv_s[...] = jnp.zeros_like(dv_s)

    dqt_s[...] = jnp.zeros_like(dqt_s)
    _stack(q_s, q_ref, heads)
    _stack(do_s, do_ref, heads)
    for n in range(heads):
        head = slice(n * HEAD, (n + 1) * HEAD)
        delta_s[:, n * BQ : (n + 1) * BQ] = (do_ref[:, head].astype(F32) * o_ref[:, head].astype(F32)).T.sum(axis=0, keepdims=True)
    gap = lax.rem(lax.broadcasted_iota(jnp.int32, (BK, 2 * BQ), 1), BQ) - lax.broadcasted_iota(jnp.int32, (BK, 2 * BQ), 0)

    def block(j, masked):
        here = pl.ds(pl.multiple_of(j * BK, BK), BK)
        k, v, kt = k_ref[here, :], v_ref[here, :], kt_s[:, here]
        pairs = range(0, heads, 2)
        cols = [slice(n * BQ, (n + 2) * BQ) for n in pairs]
        scores = [_dot(k, q_s[c, :], 1, 1) for c in cols]
        dps = [_dot(v, do_s[c, :], 1, 1) for c in cols]
        ok = gap >= j * BK - iq * BQ if masked else None
        for n, c, x, dp in zip(pairs, cols, scores, dps):
            p = jnp.exp2(x - jnp.concatenate([lse_ref[n], lse_ref[n + 1]], axis=1))
            if masked:
                p = jnp.where(ok, p, 0.0)
            ds = (p * (dp - delta_s[:, c])).astype(BF16)
            dv_s[here, :] += _dot(p.astype(BF16), do_s[c, :], 1, 0)
            dk_s[here, :] += _dot(ds, q_s[c, :], 1, 0)
            dqt_s[:, c] += _dot(kt, ds, 1, 0)

    last = lax.div(iq * BQ, BK)
    lax.fori_loop(0, last, lambda j, _: block(j, False), None)
    block(last, True)
    for n in range(heads):
        dq_ref[:, n * HEAD : (n + 1) * HEAD] = (dqt_s[:, n * BQ : (n + 1) * BQ] * SCALE).T.astype(BF16)

    @pl.when(iq == pl.num_programs(0) - 1)
    def _():
        dk_ref[...] = (dk_s[...] * LN2).astype(BF16)
        dv_ref[...] = dv_s[...].astype(BF16)


def attend_back(q, k, v, o, do, lse, carried):
    t, n = q.shape
    heads, steps = n // HEAD, t // BQ
    whole = _whole((t, HEAD))
    cols = heads * BQ
    return _call(functools.partial(_attend_back_kernel, heads=heads), "attend_back", steps,
                 [_rows(BQ, n), whole, whole, _rows(BQ, n), _rows(BQ, n), pl.BlockSpec((heads, 1, BQ), lambda i: (0, 0, i))],
                 [(_rows(BQ, n), (t, n), BF16), (whole, (t, HEAD), BF16), (whole, (t, HEAD), BF16)],
                 [pltpu.VMEM((HEAD, t), BF16), pltpu.VMEM((cols, HEAD), BF16), pltpu.VMEM((cols, HEAD), BF16), pltpu.VMEM((1, cols), F32),
                  pltpu.VMEM((HEAD, cols), F32), pltpu.VMEM((t, HEAD), F32), pltpu.VMEM((t, HEAD), F32)],
                 (q, k, v, o, do, lse), 5 * t * t * n, t * t * heads // 2, carried)


def _qkv_back_kernel(h_ref, dq_ref, dk_ref, dv_ref, c_ref, s_ref, *rest, states):
    if states:
        dh_ref, w_ref, dx_ref, dw_ref, ow_ref, w_s = rest
    else:
        dw_ref, ow_ref, w_s = rest
    i = pl.program_id(0)

    @pl.when(i == 0)
    def _():
        w_s[...] = jnp.zeros_like(w_s)

    h = h_ref[...].astype(F32)
    scale = _scale_of(h)
    a = (h * scale).astype(BF16)
    c, s = c_ref[...], s_ref[...]
    parts = [_turn_back(dq_ref[:, at : at + HEAD].astype(F32), c, s).astype(BF16) for at in range(0, dq_ref.shape[1], HEAD)]
    parts += [_turn_back(dk_ref[...].astype(F32), c, s).astype(BF16), dv_ref[...]]
    d = jnp.concatenate(parts, axis=1)
    w_s[...] += _dot(a, d, 0, 0)
    if states:
        dx_ref[...] = (dh_ref[...].astype(F32) + _norm_back(h, scale, _dot(d, w_ref[...], 1, 1))).astype(BF16)

    @pl.when(i == pl.num_programs(0) - 1)
    def _():
        dw_ref[...] = w_s[...].astype(BF16)
        _own(ow_ref, w_s)


def qkv_back(h, dq, dk, dv, c, s, group, dh=None, w=None):
    t, d = h.shape
    n = dq.shape[1] + 2 * HEAD
    r = 512
    states = dh is not None
    ins = [_rows(r, d), _rows(r, n - 2 * HEAD)] + [_rows(r, HEAD)] * 4 + ([_rows(r, d), _once((d, n))] if states else [])
    outs = ([(_rows(r, d), (t, d), BF16)] if states else []) + [(_once((d, n)), (d, n), BF16), (_once((d // group, n)), (d // group, n), F32)]
    got = _call(functools.partial(_qkv_back_kernel, states=states), "qkv_back", t // r, ins, outs, [pltpu.VMEM((d, n), F32)],
                (h, dq, dk, dv, c, s) + ((dh, w) if states else ()), (4 if states else 2) * t * d * n)
    return got if states else (None, *got)


def _first_kernel(f_ref, c_ref, s_ref, *, rows):
    place = (lax.broadcasted_iota(jnp.int32, c_ref.shape, 0) + pl.program_id(0) * rows).astype(F32)
    angle = place * f_ref[...]
    c_ref[...] = jnp.cos(angle)
    s_ref[...] = jnp.sin(angle) * jnp.where(lax.broadcasted_iota(jnp.int32, s_ref.shape, 1) < HEAD // 2, -1.0, 1.0)


def first(tokens, carried):
    half = HEAD // 2
    f = THETA ** (-jnp.arange(half, dtype=F32) / half)
    r = tokens // 4
    return _call(functools.partial(_first_kernel, rows=r), "first", 4, [_whole((1, HEAD))], [(_rows(r, HEAD), (tokens, HEAD), F32)] * 2, [],
                 (jnp.concatenate([f, f])[None],), tokens * HEAD, tokens * HEAD, carried)


def last_sums(g, n):
    rows = g.shape[0] // n
    half = rows // 2
    _, right, left, over = _places()
    part = lambda place, first: lax.dynamic_slice_in_dim(g, place * rows + first, half, 0)
    up, down = [(i, (i + 1) % n) for i in range(n)], [(i, (i - 1) % n) for i in range(n)]
    in_a, in_b = lax.ppermute(part(over, 0), "dp", up), lax.ppermute(part(over, half), "dp", down)
    b_left, a_right = lax.ppermute(part(right, half), "dp", up), lax.ppermute(part(left, 0), "dp", down)
    both = lambda x, y: (x.astype(F32) + y.astype(F32)).astype(BF16)
    a_left = lax.ppermute(both(part(right, 0), in_a), "dp", up)
    b_right = lax.ppermute(both(part(left, half), in_b), "dp", down)
    return jnp.concatenate([a_left, b_left], 0), jnp.concatenate([a_right, b_right], 0)


def adamw(w, m, v, g):
    m = 0.9 * m + 0.1 * g
    v = 0.95 * v + 0.05 * g * g
    step = m * lax.rsqrt(v + 1e-8) + 0.1 * w
    return (w - 0.02 * step).astype(BF16), m, v


def solution(mesh):
    group = mesh.shape["dp"]

    def step(x, dy, *arrays):
        weights, m, v = (arrays[i : i + 7] for i in (0, 7, 14))
        wq, wk, wv, wo, wg, wu, wd = weights
        layers = wq.shape[0]
        heads = lambda n, at: Fetch(4 * n, n, [[wq, wk, wv]], at, group)
        c, s, wa = first(x.shape[1], heads(0, (2, 3)))
        h, kept = x[0], []
        for n in range(layers):
            q, k, vv = qkv(h, wa, c, s)
            o, lse, wb, wc, we = attend(q, k, vv, Fetch(4 * n + 1, n, [[wo], [wg, wu], [wd]], (5, 7), group))
            h1, h2, *then = mlp(h, o, wb, wc, we, heads(n + 1, (2, 3)) if n + 1 < layers else None)
            kept.append((h, q, k, vv, o, lse, h1, wa, wb, wc, we))
            h, wa = h2, then[0] if then else None
        by_h, own, came, waiting = dy[0], [None] * layers, [None] * layers, None
        for n in reversed(range(layers)):
            h, q, k, vv, o, lse, h1, wa, wb, wc, we = kept[n]
            dh1, dgu, dd, ogu, od, *got = mlp_back(h1, by_h, wc, we, group, Sums(4 * n + 2, [waiting], 2, group) if n + 1 < layers else None)
            if got:
                came[n + 1] += got
            do, dwo, owo = out_back(dh1, o, wb, group)
            dq, dk, dv, *got = attend_back(q, k, vv, o, do, lse, Sums(4 * n + 3, [dwo, dgu, dd], 4, group))
            by_h, waiting, oqkv = qkv_back(h, dq, dk, dv, c, s, group, *((dh1, wa) if n else ()))
            own[n], came[n] = [owo, ogu, od, oqkv], got
        came[0] += last_sums(waiting, group)

        def sums(n):
            o, gu, d, qkv = (one + came[n][2 * i].astype(F32) + came[n][2 * i + 1].astype(F32) for i, one in enumerate(own[n]))
            a, b, ff = wq.shape[2], wk.shape[2], wg.shape[2]
            return qkv[:, :a], qkv[:, a : a + b], qkv[:, a + b :], o, gu[:, :ff], gu[:, ff:], d

        gradients = [jnp.stack(g).astype(BF16).astype(F32) for g in zip(*(sums(n) for n in range(layers)))]
        new = [adamw(w.astype(F32), m, v, g) for w, m, v, g in zip(weights, m, v, gradients, strict=True)]
        return tuple(one[which] for which in range(3) for one in new)

    states, cut = P(("rep", "dp"), None, None), P(None, "dp", None)
    return jax.shard_map(
        step,
        mesh=mesh,
        in_specs=(states, states) + (cut,) * 21,
        out_specs=(P("rep", "dp", None),) * 21,
        check_vma=False,
    )
```
